32 devices in a mesh: dp: 16 (over z, y, x), mp: 2 (over core).
Axes of the slice: x: 2, y: 2, z: 4, core: 2. Of those that a mesh axis runs over, the one named last changes fastest.
Arguments:
- inputs: bfloat16 [2048, 1792], P('dp', 'mp'), may hold values from -6 to 6
- cotangent: bfloat16 [2048, 1792], P('dp', 'mp'), may hold values from -6 to 6
- gate_weight: bfloat16 [9472, 1792], P(('mp', 'dp')), may hold values from -0.125 to 0.125
- up_weight: bfloat16 [9472, 1792], P(('mp', 'dp')), may hold values from -0.125 to 0.125
- down_weight: bfloat16 [9472, 1792], P(('mp', 'dp')), may hold values from -0.0625 to 0.0625
Outputs:
- input_grad: bfloat16 [2048, 1792], P('dp', 'mp')
- gate_grad: bfloat16 [9472, 1792], P(('mp', 'dp'))
The draws below stay inside these ranges and needn't reach their ends.
All inputs are finite; a program needn't handle non-finite values.
Results may differ from the reference program's by a relative error of at most 0.009.
Values may be sent and summed in bfloat16 or wider, within the bound.
A program may use at most 320 MiB of HBM per device.

```python
import jax
import jax.numpy as jnp
from jax import lax

D = 1792
FF = 9472
TOKENS = 2048


def levels(stream_key, shape, cuts, least, high):
    def one(dim, blocks):
        steps = jax.random.uniform(jax.random.fold_in(jax.random.fold_in(stream_key, 6), dim), (blocks,), jnp.float32, least / len(cuts), high / len(cuts))
        return jnp.repeat(jnp.exp(steps), shape[dim] // blocks).reshape((-1,) + (1,) * (len(shape) - dim - 1))

    level = one(*cuts[0])
    for cut in cuts[1:]:
        level = level * one(*cut)
    return level


def centred(own_key, extent, spread, limit, shards=(), held_as=jnp.bfloat16):
    values = jax.random.normal(own_key, extent, jnp.float32) * spread
    if len(shards) > 0:
        values = levels(own_key, extent, shards, -0.22, 0.18) * values
    return jnp.clip(values, min=-limit, max=limit).astype(held_as)


def setup_inputs(seed: int = 0) -> dict:
    streams_of = jax.random.split(jax.random.key(seed), 6)
    return {
        "inputs": centred(streams_of[0], (TOKENS, D), 1.0, 6.0, ((0, 16), (1, 2))),
        "cotangent": centred(streams_of[1], (TOKENS, D), 1.0, 6.0, ((0, 16), (1, 2))),
        "gate_weight": centred(streams_of[2], (FF, D), D ** -0.5, 0.125, ((0, 32),)),
        "up_weight": centred(streams_of[3], (FF, D), D ** -0.5, 0.125, ((0, 32),)),
        "down_weight": centred(streams_of[4], (FF, D), FF ** -0.5, 0.0625, ((0, 32),)),
    }


def tdot(left, right):
    return lax.dot_general(left, right, (((0,), (0,)), ((), ())), preferred_element_type=jnp.float32)


def rdot(left, right):
    return lax.dot_general(left, right, (((1,), (1,)), ((), ())), preferred_element_type=jnp.float32)


def reference(inputs, cotangent, gate_weight, up_weight, down_weight):
    gate = rdot(inputs, gate_weight)
    up = rdot(inputs, up_weight)
    sig = jax.nn.sigmoid(gate)
    act = gate * sig
    dhidden = rdot(cotangent, down_weight)
    dup = (dhidden * act).astype(jnp.bfloat16)
    dgate = (dhidden * up * sig * (1.0 + gate * (1.0 - sig))).astype(jnp.bfloat16)
    gate_grad = tdot(dgate, inputs).astype(jnp.bfloat16)
    input_grad = jnp.dot(dgate, gate_weight, preferred_element_type=jnp.float32)
    input_grad = input_grad + jnp.dot(dup, up_weight, preferred_element_type=jnp.float32)
    return input_grad.astype(jnp.bfloat16), gate_grad
```

```python
import jax
import jax.numpy as jnp
from jax import lax
from jax.sharding import PartitionSpec as P


def tdot(left, right):
    return lax.dot_general(
        left, right, (((0,), (0,)), ((), ())), preferred_element_type=jnp.float32
    )


def rdot(left, right):
    return lax.dot_general(
        left, right, (((1,), (1,)), ((), ())), preferred_element_type=jnp.float32
    )


def per_device(inputs, cotangent, gate_weight, up_weight, down_weight):
    def tokens(block):
        rows = lax.all_gather(block, "dp", axis=0, tiled=True)
        return lax.all_gather(rows, "mp", axis=1, tiled=True)

    full_in = tokens(inputs)
    full_cot = tokens(cotangent)
    gate = rdot(full_in, gate_weight)
    up = rdot(full_in, up_weight)
    dhidden = rdot(full_cot, down_weight)
    sig = jax.nn.sigmoid(gate)
    act = gate * sig
    dup = (dhidden * act).astype(jnp.bfloat16)
    dgate = (dhidden * up * sig * (1.0 + gate * (1.0 - sig))).astype(jnp.bfloat16)
    partial = jnp.dot(dgate, gate_weight, preferred_element_type=jnp.float32)
    partial = partial + jnp.dot(dup, up_weight, preferred_element_type=jnp.float32)
    partial = lax.psum_scatter(
        partial.astype(jnp.bfloat16), "mp", scatter_dimension=1, tiled=True
    )
    input_grad = lax.psum_scatter(partial, "dp", scatter_dimension=0, tiled=True)
    gate_grad = tdot(dgate, full_in).astype(jnp.bfloat16)
    return (input_grad, gate_grad)


def solution(mesh):
    placed = (
        P("dp", "mp"),
        P("dp", "mp"),
        P(("mp", "dp"), None),
        P(("mp", "dp"), None),
        P(("mp", "dp"), None),
    )
    return jax.shard_map(
        per_device,
        mesh=mesh,
        in_specs=placed,
        out_specs=(P("dp", "mp"), P(("mp", "dp"), None)),
        check_vma=False,
    )
```

```python
import functools

import jax
import jax.numpy as jnp
from jax import lax
from jax.experimental import pallas as pl
from jax.experimental.pallas import tpu as pltpu
from jax.sharding import PartitionSpec as P

F32 = jnp.float32
BF16 = jnp.bfloat16
VMEM_LIMIT = 63 * 1024 * 1024


def tdot(left, right):
    return lax.dot_general(
        left, right, (((0,), (0,)), ((), ())), preferred_element_type=F32
    )


def rdot(left, right):
    return lax.dot_general(
        left, right, (((1,), (1,)), ((), ())), preferred_element_type=F32
    )


def gradients(gate, up, dhidden):
    sig = jax.nn.sigmoid(gate)
    act = gate * sig
    dup = (dhidden * act).astype(BF16)
    dgate = (dhidden * up * sig * (1.0 + gate * (1.0 - sig))).astype(BF16)
    return dgate, dup


def by_collectives(inputs, cotangent, gate_weight, up_weight, down_weight):
    def tokens(block):
        rows = lax.all_gather(block, "dp", axis=0, tiled=True)
        return lax.all_gather(rows, "mp", axis=1, tiled=True)

    full_in = tokens(inputs)
    full_cot = tokens(cotangent)
    dgate, dup = gradients(
        rdot(full_in, gate_weight),
        rdot(full_in, up_weight),
        rdot(full_cot, down_weight),
    )
    partial = jnp.dot(dgate, gate_weight, preferred_element_type=F32)
    partial = partial + jnp.dot(dup, up_weight, preferred_element_type=F32)
    partial = lax.psum_scatter(
        partial.astype(BF16), "mp", scatter_dimension=1, tiled=True
    )
    input_grad = lax.psum_scatter(partial, "dp", scatter_dimension=0, tiled=True)
    return input_grad, tdot(dgate, full_in).astype(BF16)


def kernel(
    nz,
    in_ref,
    cot_ref,
    gw,
    uw,
    dw,
    ig_ref,
    gg_ref,
    tok,
    dgt,
    mine,
    give,
    took,
    r1,
    r2,
    r3,
    ag_send,
    ag_recv,
    swap_send,
    swap_recv,
    s1_send,
    s1_recv,
    s2_send,
    s2_recv,
    s3_send,
    s3_recv,
):
    rows, wide = in_ref.shape
    half_rows = rows // 2
    d = lax.axis_index("dp")
    c = lax.axis_index("mp")
    z, r = d // 4, d % 4
    y, x = r // 2, r % 2
    other = 1 - c
    own_rank = r
    x_rank, y_rank, far_rank = y * 2 + 1 - x, (1 - y) * 2 + x, (1 - y) * 2 + 1 - x
    peer, xn, yn = (d, other), (z * 4 + x_rank, c), (z * 4 + y_rank, c)

    def column(k):
        return (((z + k) % nz) * 4 + r, c)

    barrier = pltpu.get_barrier_semaphore()
    friends = [peer, xn, yn] + [column(k) for k in range(1, nz)]
    for friend in friends:
        pl.semaphore_signal(
            barrier, inc=1, device_id=friend, device_id_type=pl.DeviceIdType.MESH
        )
    pl.semaphore_wait(barrier, len(friends))

    sent = []

    def send(src, dst, send_sem, recv_sem, device):
        copy = pltpu.make_async_remote_copy(
            src_ref=src,
            dst_ref=dst,
            send_sem=send_sem,
            recv_sem=recv_sem,
            device_id=device,
            device_id_type=pl.DeviceIdType.MESH,
        )
        copy.start()
        sent.append(copy)

    def arrive(dst, send_sem, recv_sem):
        pltpu.make_async_remote_copy(
            src_ref=dst,
            dst_ref=dst,
            send_sem=send_sem,
            recv_sem=recv_sem,
            device_id=peer,
            device_id_type=pl.DeviceIdType.MESH,
        ).wait_recv()

    count = [0, 0]

    def pass_on(a, slot, device, src=None, half=c):
        src = tok.at[a, half, slot] if src is None else src
        send(
            src,
            tok.at[a, half, slot],
            ag_send.at[a, count[a]],
            ag_recv.at[a, half, slot],
            device,
        )
        count[a] += 1

    def landed(a, half, slot):
        arrive(tok.at[a, half, slot], ag_send.at[a, 0], ag_recv.at[a, half, slot])

    sources = (in_ref, cot_ref)
    first, second = (xn, yn), (yn, xn)
    first_rank, second_rank = (x_rank, y_rank), (y_rank, x_rank)

    def layer(k):
        return (z + nz - k) % nz

    for a in range(2):
        pass_on(a, d, first[a], sources[a])
    for k in range(1, nz):
        for a in range(2):
            pass_on(a, d, column(k), sources[a])
    for a in range(2):
        pass_on(a, d, second[a], sources[a])
    for a in range(2):
        pass_on(a, d, peer, sources[a])
    for a in range(2):
        tok[a, c, d] = sources[a][...]

    def from_column(k):
        slot = layer(k) * 4 + own_rank
        for a in range(2):
            landed(a, c, slot)
            pass_on(a, slot, first[a])
            pass_on(a, slot, second[a])
            pass_on(a, slot, peer)

    def from_first(k):
        for a in range(2):
            slot = layer(k) * 4 + first_rank[a]
            landed(a, c, slot)
            pass_on(a, slot, second[a])
            pass_on(a, slot, peer)

    def from_second(k):
        for a in range(2):
            slot = layer(k) * 4 + second_rank[a]
            landed(a, c, slot)
            pass_on(a, slot, peer)
        for a in range(2):
            slot = layer(k) * 4 + far_rank
            landed(a, c, slot)
            pass_on(a, slot, peer)

    own_columns = pl.ds(pl.multiple_of(c * wide, 128), wide)
    other_columns = pl.ds(pl.multiple_of(other * wide, 128), wide)

    def compute(k):
        base = layer(k) * 4
        for rank in (own_rank, x_rank, y_rank, far_rank):
            for a in range(2):
                landed(a, other, base + rank)

        @pl.loop(0, 2)
        def _(j):
            s = base + 2 * j

            def project(weight, a):
                total = None
                for h in range(2):
                    block = tok[a, h, pl.ds(s, 2)].reshape(2 * rows, wide)
                    part = rdot(weight[:, h * wide : (h + 1) * wide], block)
                    total = part if total is None else total + part
                return total

            dgate, dup = gradients(project(gw, 0), project(uw, 0), project(dw, 1))
            dgt[:, pl.ds(pl.multiple_of(s * rows, 128), 2 * rows)] = dgate
            for target, columns in ((give, other_columns), (mine, own_columns)):
                part = tdot(dgate, gw[:, columns]) + tdot(dup, uw[:, columns])
                target[pl.ds(s, 2)] = part.astype(BF16).reshape(2, rows, wide)

        group = pl.ds(base, 4)
        send(give.at[group], took.at[group], swap_send.at[k], swap_recv.at[k], peer)

    top, low = pl.ds(0, half_rows), pl.ds(half_rows, half_rows)

    def add(buffer, extra, slot, part):
        total = buffer[slot, part].astype(F32) + extra[slot, part].astype(F32)
        buffer[slot, part] = total.astype(BF16)

    def stage1(k):
        base = layer(k) * 4
        group = pl.ds(base, 4)
        arrive(took.at[group], swap_send.at[k], swap_recv.at[k])

        @pl.loop(0, 4)
        def _(j):
            add(mine, took, base + j, pl.ds(0, rows))

        for i, (part, ranks, device) in enumerate(
            ((top, (far_rank, x_rank), xn), (low, (far_rank, y_rank), yn))
        ):
            for n, rank in enumerate(ranks):
                piece = (base + rank, part)
                send(
                    mine.at[piece],
                    r1.at[piece],
                    s1_send.at[k, i, n],
                    s1_recv.at[k, i, n],
                    device,
                )

    def stage2(k):
        base = layer(k) * 4
        for n in range(2):
            for i, (part, far, device) in enumerate(
                ((top, y_rank, yn), (low, x_rank, xn))
            ):
                piece = (base + (far, own_rank)[n], part)
                arrive(r1.at[piece], s1_send.at[k, i, n], s1_recv.at[k, i, n])
                add(mine, r1, *piece)
                if n == 0:
                    send(
                        mine.at[piece],
                        r2.at[piece],
                        s2_send.at[k, i],
                        s2_recv.at[k, i],
                        device,
                    )

    def stage3(k):
        slot = layer(k) * 4 + own_rank
        for i, part in enumerate((top, low)):
            arrive(r2.at[slot, part], s2_send.at[k, i], s2_recv.at[k, i])
            add(mine, r2, slot, part)
        if k > 0:
            send(
                mine.at[slot],
                r3.at[k],
                s3_send.at[k],
                s3_recv.at[k],
                ((z + nz - k) % nz * 4 + r, c),
            )

    def weight_gradient(h):
        block = tok[0, h].reshape(-1, wide)
        grad = jnp.dot(dgt[...], block, preferred_element_type=F32)
        gg_ref[:, h * wide : (h + 1) * wide] = grad.astype(BF16)

    for k in range(nz):
        from_first(k)
        if k + 1 < nz:
            from_column(k + 1)
        from_second(k)
        if k >= 1:
            stage1(k - 1)
        if k >= 2:
            stage2(k - 2)
        if k >= 3:
            stage3(k - 3)
        compute(k)
    last = nz - 1
    if nz >= 2:
        stage2(last - 1)
    if nz >= 3:
        stage3(last - 2)
    stage1(last)
    if nz >= 2:
        stage3(last - 1)
    weight_gradient(0)
    stage2(last)
    weight_gradient(1)
    stage3(last)
    total = mine[d].astype(F32)
    for k in range(1, nz):
        arrive(r3.at[k], s3_send.at[k], s3_recv.at[k])
        total = total + r3[k].astype(F32)
    ig_ref[...] = total.astype(BF16)
    for copy in sent:
        copy.wait_send()


def by_kernel(n, inputs, cotangent, gate_weight, up_weight, down_weight):
    rows, wide = inputs.shape
    hidden, features = gate_weight.shape
    nz = n // 4
    sends = 2 * n
    dma = pltpu.SemaphoreType.DMA
    whole = pltpu.VMEM((n, rows, wide), BF16)
    return pl.pallas_call(
        functools.partial(kernel, nz),
        out_shape=(
            jax.ShapeDtypeStruct((rows, wide), BF16),
            jax.ShapeDtypeStruct((hidden, features), BF16),
        ),
        in_specs=[pl.BlockSpec(memory_space=pltpu.VMEM)] * 5,
        out_specs=[pl.BlockSpec(memory_space=pltpu.VMEM)] * 2,
        scratch_shapes=[
            pltpu.VMEM((2, 2, n, rows, wide), BF16),
            pltpu.VMEM((hidden, n * rows), BF16),
            whole,
            whole,
            whole,
            whole,
            whole,
            pltpu.VMEM((nz, rows, wide), BF16),
            dma((2, sends)),
            dma((2, 2, n)),
            dma((nz,)),
            dma((nz,)),
            dma((nz, 2, 2)),
            dma((nz, 2, 2)),
            dma((nz, 2)),
            dma((nz, 2)),
            dma((nz,)),
            dma((nz,)),
        ],
        compiler_params=pltpu.CompilerParams(
            collective_id=0, has_side_effects=True, vmem_limit_bytes=VMEM_LIMIT
        ),
    )(inputs, cotangent, gate_weight, up_weight, down_weight)


def solution(mesh):
    n, cores = mesh.shape["dp"], mesh.shape["mp"]

    def per_device(inputs, cotangent, gate_weight, up_weight, down_weight):
        rows, wide = inputs.shape
        hidden, features = gate_weight.shape
        held = 2 * (9 * n * rows * wide + 5 * hidden * features + hidden * n * rows)
        fits = held <= VMEM_LIMIT * 3 // 4
        even = n % 4 == 0 and rows % 64 == 0 and wide % 128 == 0
        args = (inputs, cotangent, gate_weight, up_weight, down_weight)
        if cores == 2 and fits and even:
            return tuple(by_kernel(n, *args))
        return by_collectives(*args)

    placed = (
        P("dp", "mp"),
        P("dp", "mp"),
        P(("mp", "dp"), None),
        P(("mp", "dp"), None),
        P(("mp", "dp"), None),
    )
    return jax.shard_map(
        per_device,
        mesh=mesh,
        in_specs=placed,
        out_specs=(P("dp", "mp"), P(("mp", "dp"), None)),
        check_vma=False,
    )
```

```python
import functools

import jax
import jax.numpy as jnp
from jax import lax
from jax.experimental import pallas as pl
from jax.experimental.pallas import tpu as pltpu
from jax.sharding import PartitionSpec as P

F32 = jnp.float32
BF16 = jnp.bfloat16
VMEM_LIMIT = 63 * 1024 * 1024


def tdot(left, right):
    return lax.dot_general(
        left, right, (((0,), (0,)), ((), ())), preferred_element_type=F32
    )


def rdot(left, right):
    return lax.dot_general(
        left, right, (((1,), (1,)), ((), ())), preferred_element_type=F32
    )


def gradients(gate, up, dhidden):
    sig = jax.nn.sigmoid(gate)
    act = gate * sig
    dup = (dhidden * act).astype(BF16)
    dgate = (dhidden * up * sig * (1.0 + gate * (1.0 - sig))).astype(BF16)
    return dgate, dup


def by_collectives(inputs, cotangent, gate_weight, up_weight, down_weight):
    def tokens(block):
        rows = lax.all_gather(block, "dp", axis=0, tiled=True)
        return lax.all_gather(rows, "mp", axis=1, tiled=True)

    full_in = tokens(inputs)
    full_cot = tokens(cotangent)
    dgate, dup = gradients(
        rdot(full_in, gate_weight),
        rdot(full_in, up_weight),
        rdot(full_cot, down_weight),
    )
    partial = jnp.dot(dgate, gate_weight, preferred_element_type=F32)
    partial = partial + jnp.dot(dup, up_weight, preferred_element_type=F32)
    partial = lax.psum_scatter(
        partial.astype(BF16), "mp", scatter_dimension=1, tiled=True
    )
    input_grad = lax.psum_scatter(partial, "dp", scatter_dimension=0, tiled=True)
    return input_grad, tdot(dgate, full_in).astype(BF16)


def kernel(
    nz,
    in_ref,
    cot_ref,
    gw_ref,
    uw_ref,
    dw_ref,
    ig_ref,
    gg_ref,
    gw,
    uw,
    dw,
    tok,
    dgt,
    mine,
    give,
    took,
    r1,
    r2,
    r3,
    ag_send,
    ag_recv,
    swap_send,
    swap_recv,
    s1_send,
    s1_recv,
    s2_send,
    s2_recv,
    s3_send,
    s3_recv,
    load_sem,
):
    rows, wide = in_ref.shape
    half_rows = rows // 2
    d = lax.axis_index("dp")
    c = lax.axis_index("mp")
    z, r = d // 4, d % 4
    y, x = r // 2, r % 2
    other = 1 - c
    own_rank = r
    x_rank, y_rank, far_rank = y * 2 + 1 - x, (1 - y) * 2 + x, (1 - y) * 2 + 1 - x
    peer, xn, yn = (d, other), (z * 4 + x_rank, c), (z * 4 + y_rank, c)

    def column(k):
        return (((z + k) % nz) * 4 + r, c)

    loads = [
        pltpu.make_async_copy(source, held, load_sem.at[i])
        for i, (source, held) in enumerate(((gw_ref, gw), (uw_ref, uw), (dw_ref, dw)))
    ]
    for load in loads:
        load.start()

    barrier = pltpu.get_barrier_semaphore()
    friends = [peer, xn, yn] + [column(k) for k in range(1, nz)]
    for friend in friends:
        pl.semaphore_signal(
            barrier, inc=1, device_id=friend, device_id_type=pl.DeviceIdType.MESH
        )
    pl.semaphore_wait(barrier, len(friends))

    sent = []

    def send(src, dst, send_sem, recv_sem, device):
        copy = pltpu.make_async_remote_copy(
            src_ref=src,
            dst_ref=dst,
            send_sem=send_sem,
            recv_sem=recv_sem,
            device_id=device,
            device_id_type=pl.DeviceIdType.MESH,
        )
        copy.start()
        sent.append(copy)

    def arrive(dst, send_sem, recv_sem):
        pltpu.make_async_remote_copy(
            src_ref=dst,
            dst_ref=dst,
            send_sem=send_sem,
            recv_sem=recv_sem,
            device_id=peer,
            device_id_type=pl.DeviceIdType.MESH,
        ).wait_recv()

    count = [0, 0]

    def pass_on(a, slot, device, src=None, half=c):
        src = tok.at[a, half, slot] if src is None else src
        send(
            src,
            tok.at[a, half, slot],
            ag_send.at[a, count[a]],
            ag_recv.at[a, half, slot],
            device,
        )
        count[a] += 1

    def landed(a, half, slot):
        arrive(tok.at[a, half, slot], ag_send.at[a, 0], ag_recv.at[a, half, slot])

    sources = (in_ref, cot_ref)
    first, second = (xn, yn), (yn, xn)
    first_rank, second_rank = (x_rank, y_rank), (y_rank, x_rank)

    def layer(k):
        return (z + nz - k) % nz

    for a in range(2):
        pass_on(a, d, first[a], sources[a])
    for k in range(1, nz):
        for a in range(2):
            pass_on(a, d, column(k), sources[a])
    for a in range(2):
        pass_on(a, d, second[a], sources[a])
    for a in range(2):
        pass_on(a, d, peer, sources[a])
    for a in range(2):
        tok[a, c, d] = sources[a][...]

    def from_column(k):
        slot = layer(k) * 4 + own_rank
        for a in range(2):
            landed(a, c, slot)
            pass_on(a, slot, first[a])
            pass_on(a, slot, second[a])
            pass_on(a, slot, peer)

    def from_first(k):
        for a in range(2):
            slot = layer(k) * 4 + first_rank[a]
            landed(a, c, slot)
            pass_on(a, slot, second[a])
            pass_on(a, slot, peer)

    def from_second(k):
        for a in range(2):
            slot = layer(k) * 4 + second_rank[a]
            landed(a, c, slot)
            pass_on(a, slot, peer)
        for a in range(2):
            slot = layer(k) * 4 + far_rank
            landed(a, c, slot)
            pass_on(a, slot, peer)

    own_columns = pl.ds(pl.multiple_of(c * wide, 128), wide)
    other_columns = pl.ds(pl.multiple_of(other * wide, 128), wide)

    def compute(k):
        base = layer(k) * 4
        for rank in (own_rank, x_rank, y_rank, far_rank):
            for a in range(2):
                landed(a, other, base + rank)

        @pl.loop(0, 2)
        def _(j):
            s = base + 2 * j

            def project(weight, a):
                total = None
                for h in range(2):
                    block = tok[a, h, pl.ds(s, 2)].reshape(2 * rows, wide)
                    part = rdot(weight[:, h * wide : (h + 1) * wide], block)
                    total = part if total is None else total + part
                return total

            dgate, dup = gradients(project(gw, 0), project(uw, 0), project(dw, 1))
            dgt[:, pl.ds(pl.multiple_of(s * rows, 128), 2 * rows)] = dgate
            for target, columns in ((give, other_columns), (mine, own_columns)):
                part = tdot(dgate, gw[:, columns]) + tdot(dup, uw[:, columns])
                target[pl.ds(s, 2)] = part.astype(BF16).reshape(2, rows, wide)

        group = pl.ds(base, 4)
        send(give.at[group], took.at[group], swap_send.at[k], swap_recv.at[k], peer)

    top, low = pl.ds(0, half_rows), pl.ds(half_rows, half_rows)

    def add(buffer, extra, slot, part):
        total = buffer[slot, part].astype(F32) + extra[slot, part].astype(F32)
        buffer[slot, part] = total.astype(BF16)

    def stage1(k):
        base = layer(k) * 4
        group = pl.ds(base, 4)
        arrive(took.at[group], swap_send.at[k], swap_recv.at[k])

        @pl.loop(0, 4)
        def _(j):
            add(mine, took, base + j, pl.ds(0, rows))

        for i, (part, ranks, device) in enumerate(
            ((top, (far_rank, x_rank), xn), (low, (far_rank, y_rank), yn))
        ):
            for n, rank in enumerate(ranks):
                piece = (base + rank, part)
                send(
                    mine.at[piece],
                    r1.at[piece],
                    s1_send.at[k, i, n],
                    s1_recv.at[k, i, n],
                    device,
                )

    def stage2(k):
        base = layer(k) * 4
        for n in range(2):
            for i, (part, far, device) in enumerate(
                ((top, y_rank, yn), (low, x_rank, xn))
            ):
                piece = (base + (far, own_rank)[n], part)
                arrive(r1.at[piece], s1_send.at[k, i, n], s1_recv.at[k, i, n])
                add(mine, r1, *piece)
                if n == 0:
                    send(
                        mine.at[piece],
                        r2.at[piece],
                        s2_send.at[k, i],
                        s2_recv.at[k, i],
                        device,
                    )

    def stage3(k):
        slot = layer(k) * 4 + own_rank
        for i, part in enumerate((top, low)):
            arrive(r2.at[slot, part], s2_send.at[k, i], s2_recv.at[k, i])
            add(mine, r2, slot, part)
        if k > 0:
            send(
                mine.at[slot],
                r3.at[k],
                s3_send.at[k],
                s3_recv.at[k],
                ((z + nz - k) % nz * 4 + r, c),
            )

    def weight_gradient(h):
        block = tok[0, h].reshape(-1, wide)
        grad = jnp.dot(dgt[...], block, preferred_element_type=F32)
        gg_ref[:, h * wide : (h + 1) * wide] = grad.astype(BF16)

    for k in range(nz):
        from_first(k)
        if k + 1 < nz:
            from_column(k + 1)
        from_second(k)
        if k >= 1:
            stage1(k - 1)
        if k >= 2:
            stage2(k - 2)
        if k >= 3:
            stage3(k - 3)
        if k == 0:
            for load in loads:
                load.wait()
        compute(k)
    last = nz - 1
    if nz >= 2:
        stage2(last - 1)
    if nz >= 3:
        stage3(last - 2)
    stage1(last)
    if nz >= 2:
        stage3(last - 1)
    weight_gradient(0)
    stage2(last)
    weight_gradient(1)
    stage3(last)
    total = mine[d].astype(F32)
    for k in range(1, nz):
        arrive(r3.at[k], s3_send.at[k], s3_recv.at[k])
        total = total + r3[k].astype(F32)
    ig_ref[...] = total.astype(BF16)
    for copy in sent:
        copy.wait_send()


def by_kernel(n, inputs, cotangent, gate_weight, up_weight, down_weight):
    rows, wide = inputs.shape
    hidden, features = gate_weight.shape
    nz = n // 4
    sends = 2 * n
    dma = pltpu.SemaphoreType.DMA
    whole = pltpu.VMEM((n, rows, wide), BF16)
    return pl.pallas_call(
        functools.partial(kernel, nz),
        out_shape=(
            jax.ShapeDtypeStruct((rows, wide), BF16),
            jax.ShapeDtypeStruct((hidden, features), BF16),
        ),
        in_specs=[pl.BlockSpec(memory_space=pltpu.VMEM)] * 2
        + [pl.BlockSpec(memory_space=pl.ANY)] * 3,
        out_specs=[pl.BlockSpec(memory_space=pltpu.VMEM)] * 2,
        scratch_shapes=[pltpu.VMEM((hidden, features), BF16)] * 3
        + [
            pltpu.VMEM((2, 2, n, rows, wide), BF16),
            pltpu.VMEM((hidden, n * rows), BF16),
            whole,
            whole,
            whole,
            whole,
            whole,
            pltpu.VMEM((nz, rows, wide), BF16),
            dma((2, sends)),
            dma((2, 2, n)),
            dma((nz,)),
            dma((nz,)),
            dma((nz, 2, 2)),
            dma((nz, 2, 2)),
            dma((nz, 2)),
            dma((nz, 2)),
            dma((nz,)),
            dma((nz,)),
            dma((3,)),
        ],
        compiler_params=pltpu.CompilerParams(
            collective_id=0, has_side_effects=True, vmem_limit_bytes=VMEM_LIMIT
        ),
    )(inputs, cotangent, gate_weight, up_weight, down_weight)


def solution(mesh):
    n, cores = mesh.shape["dp"], mesh.shape["mp"]

    def per_device(inputs, cotangent, gate_weight, up_weight, down_weight):
        rows, wide = inputs.shape
        hidden, features = gate_weight.shape
        held = 2 * (9 * n * rows * wide + 5 * hidden * features + hidden * n * rows)
        fits = held <= VMEM_LIMIT * 3 // 4
        even = n % 4 == 0 and rows % 64 == 0 and wide % 128 == 0
        args = (inputs, cotangent, gate_weight, up_weight, down_weight)
        if cores == 2 and fits and even:
            return tuple(by_kernel(n, *args))
        return by_collectives(*args)

    placed = (
        P("dp", "mp"),
        P("dp", "mp"),
        P(("mp", "dp"), None),
        P(("mp", "dp"), None),
        P(("mp", "dp"), None),
    )
    return jax.shard_map(
        per_device,
        mesh=mesh,
        in_specs=placed,
        out_specs=(P("dp", "mp"), P(("mp", "dp"), None)),
        check_vma=False,
    )
```
